256 devices in a mesh: mp: 64 (over z, x, core), head: 4 (over y).
Axes of the slice: x: 4, y: 4, z: 8, core: 2. Of those that a mesh axis runs over, the one named last changes fastest.
Arguments:
- hidden: bfloat16 [8, 4096], replicated, may hold values from -6 to 6
- norm_gain: float32 [4096], replicated, may hold values from 0.25 to 1.75
- w_query: bfloat16 [4096, 4096], P('mp', 'head'), may hold values from -0.09375 to 0.09375
- enc_states: bfloat16 [8, 4096, 4096], P(None, 'mp'), may hold values from -6 to 6
- w_key: bfloat16 [4096, 4096], P('mp', 'head'), may hold values from -0.09375 to 0.09375
- w_value: bfloat16 [4096, 4096], P('mp', 'head'), may hold values from -0.09375 to 0.09375
- w_out: bfloat16 [4096, 4096], P('head', 'mp'), may hold values from -0.09375 to 0.09375
- bias_table: float32 [32, 64], P(None, 'head'), may hold values from -5 to 300
- buckets: int32 [8, 4096], P(None, 'mp'), may hold values from 0 to 31
- src_len: int32 [8], replicated, may hold values from 512 to 4096
Outputs:
- updated: bfloat16 [8, 4096], P(None, 'mp')
The draws below stay inside these ranges and needn't reach their ends.
All inputs are finite; a program needn't handle non-finite values.
Results may differ from the reference program's by a relative error of at most 0.0049.
Values may be sent and summed in bfloat16 or wider, within the bound.
A program may use at most 128 MiB of HBM per device.

```python
import jax
import jax.numpy as jnp
from jax import lax

D = 4096
HEADS = 64
DH = 64
BUCKETS = 32
BATCH = 8
INNER = 4096
S = 4096


def draw_bias_table(key, part):
    base_key = jax.random.fold_in(jax.random.fold_in(key, 7), 0)
    result = jnp.clip(jax.random.normal(base_key, (BUCKETS, HEADS), jnp.float32), -5.0, 5.0)
    return result


def place_ends(drawn, rng, smallest, largest):
    spot = [jax.random.randint(jax.random.fold_in(rng, axis), (), 0, length) for axis, length in enumerate(drawn.shape)]
    longest = drawn.shape.index(max(drawn.shape))
    next_to = spot[:longest] + [(spot[longest] + 1) % drawn.shape[longest]] + spot[longest + 1:]
    return drawn.at[tuple(spot)].set(smallest).at[tuple(next_to)].set(largest)


def shard_levels(own_key, dims, cuts, least, largest):
    gain, own = 1.0, jax.random.fold_in(own_key, 6)
    for dim, shards_of in cuts:
        heights = jnp.exp(jax.random.uniform(jax.random.fold_in(own, dim), (shards_of,), jnp.float32, least / len(cuts), largest / len(cuts)))
        gain = gain * jnp.repeat(heights, dims[dim] // shards_of).reshape([-1 if axis == dim else 1 for axis in range(len(dims))])
    return gain


def centred(key, shape, width, most, pieces=(), kind=jnp.bfloat16):
    entries = width * jax.random.normal(key, shape, jnp.float32)
    if pieces:
        entries = entries * shard_levels(key, shape, pieces, -0.22, 0.18)
    return jnp.clip(entries, -most, most).astype(kind)


def setup_inputs(seed: int = 0) -> dict:
    splits = jax.random.split(jax.random.key(seed), 11)
    return {
        "hidden": centred(splits[0], (BATCH, D), 1.0, 6.0),
        "norm_gain": jnp.clip(1.0 + 0.15 * jax.random.normal(splits[1], (D,), jnp.float32), 0.25, 1.75),
        "w_query": centred(splits[2], (D, INNER), D ** -0.5, 0.09375, ((0, 64), (1, 4))),
        "enc_states": centred(splits[3], (BATCH, S, D), 1.0, 6.0, ((1, 64),)),
        "w_key": centred(splits[4], (D, INNER), D ** -0.5, 0.09375, ((0, 64), (1, 4))),
        "w_value": centred(splits[5], (D, INNER), D ** -0.5, 0.09375, ((0, 64), (1, 4))),
        "w_out": centred(splits[6], (INNER, D), INNER ** -0.5, 0.09375, ((0, 4), (1, 64))),
        "bias_table": draw_bias_table(jax.random.fold_in(splits[10], 71), 0),
        "buckets": place_ends(jax.random.randint(splits[8], (BATCH, S), 0, BUCKETS), jax.random.fold_in(splits[8], 1), 0, BUCKETS - 1).astype(jnp.int32),
        "src_len": place_ends(jax.random.randint(splits[9], (BATCH,), S // 8, S + 1), jax.random.fold_in(splits[9], 1), S // 8, S).astype(jnp.int32),
    }


EPSILON = 1e-06
NEGATIVE = -1e+30

def reference(hidden, norm_gain, w_query, enc_states, w_key, w_value, w_out, bias_table, buckets, src_len):
    widened = hidden.astype(jnp.float32)
    mean_square = lax.optimization_barrier(jnp.mean(widened * widened, axis=-1, keepdims=True))
    normed = (widened * lax.rsqrt(mean_square + EPSILON) * norm_gain.astype(jnp.float32)).astype(jnp.bfloat16)
    query = jnp.dot(normed, w_query, preferred_element_type=jnp.float32).astype(jnp.bfloat16)
    query = query.reshape(BATCH, HEADS, DH)
    flat_rows = enc_states.reshape(BATCH * S, D)
    key_rows = jnp.dot(flat_rows, w_key, preferred_element_type=jnp.float32)
    value_rows = jnp.dot(flat_rows, w_value, preferred_element_type=jnp.float32)
    key_rows = key_rows.reshape(BATCH, S, HEADS, DH)
    value_rows = value_rows.reshape(BATCH, S, HEADS, DH)
    factor = float(DH) ** (-0.5)
    scores = jnp.einsum('bhd,bshd->bhs', query.astype(jnp.float32), key_rows, precision=lax.Precision.HIGHEST) * factor
    scores = scores + jnp.transpose(bias_table[buckets], (0, 2, 1))
    is_live = (jnp.arange(S, dtype=jnp.int32)[None, :] < src_len[:, None])[:, None, :]
    scores = jnp.where(is_live, scores, NEGATIVE)
    best_max = lax.optimization_barrier(jnp.max(scores, axis=-1, keepdims=True))
    weights = jnp.where(is_live, jnp.exp(scores - best_max), 0.0)
    denominator = lax.optimization_barrier(jnp.sum(weights, axis=-1))
    weighted = jnp.einsum('bhs,bshd->bhd', weights, value_rows, precision=lax.Precision.HIGHEST)
    context = (weighted / denominator[:, :, None]).reshape(BATCH, INNER).astype(jnp.bfloat16)
    projected = jnp.dot(context, w_out, preferred_element_type=jnp.float32)
    return (projected + widened).astype(jnp.bfloat16)
```

```python
import jax
import jax.numpy as jnp
from jax import lax
from jax.sharding import PartitionSpec as P

EPSILON = 1e-06
NEGATIVE = -1e30


def shards(
    hidden, norm_gain, w_query, enc_states, w_key, w_value, w_out, bias_table, buckets, src_len
):
    batch, src_local, _ = enc_states.shape
    rows, inner = w_key.shape
    heads = bias_table.shape[1]
    head_size = inner // heads
    me = lax.axis_index("mp")
    widened = hidden.astype(jnp.float32)
    mean_square = jnp.mean(widened * widened, axis=-1, keepdims=True)
    normed = (widened * lax.rsqrt(mean_square + EPSILON) * norm_gain).astype(jnp.bfloat16)
    mine = lax.dynamic_slice_in_dim(normed, me * rows, rows, 1)
    query = jnp.dot(mine, w_query, preferred_element_type=jnp.float32)
    query = lax.psum(query, "mp").astype(jnp.bfloat16).reshape(batch, heads, head_size)
    probe = jnp.einsum(
        "bhe,dhe->bhd",
        query,
        w_key.reshape(rows, heads, head_size),
        preferred_element_type=jnp.float32,
    )
    probe = (probe * float(head_size) ** (-0.5)).astype(jnp.bfloat16)
    probe = lax.all_gather(probe, "mp", axis=2, tiled=True)
    scores = jnp.einsum("bhd,bsd->bhs", probe, enc_states, preferred_element_type=jnp.float32)
    ids = jnp.arange(bias_table.shape[0], dtype=jnp.int32)
    one_hot = (buckets[:, :, None] == ids[None, None, :]).astype(jnp.float32)
    scores = scores + jnp.einsum(
        "bsk,kh->bhs", one_hot, bias_table, precision=lax.Precision.HIGHEST
    )
    positions = me * src_local + jnp.arange(src_local, dtype=jnp.int32)
    live = (positions[None, :] < src_len[:, None])[:, None, :]
    scores = jnp.where(live, scores, NEGATIVE)
    top = lax.pmax(jnp.max(scores, axis=-1), "mp")
    weights = jnp.where(live, jnp.exp(scores - top[:, :, None]), 0.0)
    total = lax.psum(jnp.sum(weights, axis=-1), "mp")
    mixed = jnp.einsum(
        "bhs,bsd->bhd",
        weights.astype(jnp.bfloat16),
        enc_states,
        preferred_element_type=jnp.float32,
    )
    mixed = lax.psum_scatter(mixed, "mp", scatter_dimension=2, tiled=True)
    mixed = (mixed / total[:, :, None]).astype(jnp.bfloat16)
    context = jnp.einsum(
        "bhd,dhe->bhe",
        mixed,
        w_value.reshape(rows, heads, head_size),
        preferred_element_type=jnp.float32,
    )
    context = lax.psum(context, "mp").astype(jnp.bfloat16).reshape(batch, inner)
    out = lax.psum(jnp.dot(context, w_out, preferred_element_type=jnp.float32), "head")
    cols = w_out.shape[1]
    residual = lax.dynamic_slice_in_dim(widened, me * cols, cols, 1)
    return (out + residual).astype(jnp.bfloat16)


def solution(mesh):
    in_specs = (
        P(),
        P(),
        P("mp", "head"),
        P(None, "mp", None),
        P("mp", "head"),
        P("mp", "head"),
        P("head", "mp"),
        P(None, "head"),
        P(None, "mp"),
        P(),
    )
    return jax.shard_map(
        shards, mesh=mesh, in_specs=in_specs, out_specs=P(None, "mp"), check_vma=False
    )
```

```python
import functools

import jax
import jax.numpy as jnp
from jax import lax
from jax.experimental import pallas as pl
from jax.experimental.pallas import tpu as pltpu
from jax.sharding import PartitionSpec as P

EPSILON = 1e-06
NEGATIVE = -1e30
NX = 4
NC = 2
LANES = 128
MESH = pl.DeviceIdType.MESH
F32 = jnp.float32
BF16 = jnp.bfloat16
NT = (((1,), (1,)), ((), ()))


def split3(value):
    first = value.astype(BF16).astype(F32)
    second = (value - first).astype(BF16).astype(F32)
    return first, second, value - first - second


def pack_stats(top, total):
    parts = split3(top) + split3(total)
    lane = lax.broadcasted_iota(jnp.int32, (top.shape[0], LANES), 1) // 16
    out = jnp.zeros((top.shape[0], LANES), F32)
    for k, part in enumerate(parts):
        out = jnp.where(lane == k, part, out)
    return out


def unpack_stats(stats):
    col = [stats[:, 16 * k : 16 * k + 1] for k in range(6)]
    return col[0] + col[1] + col[2], col[3] + col[4] + col[5]


def opened(block, width):
    block = block.astype(F32)
    return (block[:, :width], *unpack_stats(block[:, width:]))


def merged(parts):
    top = functools.reduce(jnp.maximum, [p[1] for p in parts])
    scales = [jnp.exp(p[1] - top) for p in parts]
    data = functools.reduce(jnp.add, [p[0] * s for p, s in zip(parts, scales)])
    total = functools.reduce(jnp.add, [p[2] * s for p, s in zip(parts, scales)])
    return data, top, total


def closed(part):
    data, top, total = part
    return jnp.concatenate([data, pack_stats(top, total)], axis=1).astype(BF16)


def kernel(
    nz,
    ny,
    n_send,
    n_recv,
    table,
    src_len,
    hidden,
    gain,
    w_query,
    enc,
    w_key,
    w_value,
    w_out,
    buckets,
    out,
    hid_v,
    gain_v,
    wq_v,
    wo_v,
    bk_v,
    enc_v,
    kw,
    vw,
    qz,
    qx,
    probe,
    add_v,
    mix,
    sib,
    half,
    hop,
    zsend,
    zrecv,
    cx,
    cz,
    yo,
    local_sem,
    enc_sem,
    send_sem,
    recv_sem,
):
    batch = hid_v.shape[0]
    width = nz * LANES
    me = lax.axis_index("mp")
    my_y = lax.axis_index("head")
    z = me // (NX * NC)
    x = lax.rem(me // NC, NX)
    c = lax.rem(me, NC)
    other = 1 - c

    def mp_of(zz, xx, cc):
        return (zz * NX + xx) * NC + cc

    def zat(dz):
        return lax.rem(z + dz, nz)

    def xat(dx):
        return lax.rem(x + dx, NX)

    far = sorted(range(1, nz), key=lambda d: -min(d, nz - d))
    near = far[::-1]
    sends = []
    counts = {"send": 0, "recv": 0}

    def fresh(kind, number):
        first = counts[kind]
        counts[kind] += number
        return first

    def copy_to(src, dst, recv, device):
        copy = pltpu.make_async_remote_copy(
            src_ref=src,
            dst_ref=dst,
            send_sem=send_sem.at[fresh("send", 1)],
            recv_sem=recv_sem.at[recv],
            device_id=device,
            device_id_type=MESH,
        )
        copy.start()
        sends.append(copy)

    def landed(dst, recv):
        pltpu.make_async_remote_copy(
            src_ref=dst,
            dst_ref=dst,
            send_sem=send_sem.at[0],
            recv_sem=recv_sem.at[recv],
            device_id={"mp": me},
            device_id_type=MESH,
        ).wait_recv()

    def mp(zz, xx, cc):
        return {"mp": mp_of(zz, xx, cc)}

    barrier = pltpu.get_barrier_semaphore()
    peers = [mp(z, xat(dx), cc) for dx in range(1, NX) for cc in (0, 1)]
    peers += [mp(z, x, other)]
    peers += [mp(zat(dz), x, cc) for dz in far for cc in (0, 1)]
    peers += [{"head": lax.rem(my_y + dy, ny)} for dy in range(1, ny)]
    for peer in peers:
        pl.semaphore_signal(barrier, inc=1, device_id=peer, device_id_type=MESH)

    local = [
        pltpu.make_async_copy(src, dst, local_sem.at[k])
        for k, (src, dst) in enumerate(
            [
                (hidden, hid_v),
                (w_query, wq_v),
                (gain, gain_v),
                (buckets, bk_v),
                (w_out, wo_v),
                (w_key.at[:, pl.ds(pl.multiple_of(z * LANES, LANES), LANES)], kw.at[z, c]),
                (w_value.at[:, pl.ds(pl.multiple_of(z * LANES, LANES), LANES)], vw.at[z, c]),
            ]
        )
    ]
    for copy in local:
        copy.start()
    for xx in range(NX):
        for zz in range(nz):
            pltpu.make_async_copy(
                enc.at[:, pl.ds(zz * NX * LANES + xx * LANES, LANES)],
                enc_v.at[xx, :, pl.ds(zz * LANES, LANES)],
                enc_sem.at[xx],
            ).start()

    local[0].wait()
    wide = hid_v[...].astype(F32)
    mean_square = jnp.mean(wide * wide, axis=-1, keepdims=True)
    local[2].wait()
    lanes_of = pl.ds(pl.multiple_of((z * NX + x) * LANES, LANES), LANES)
    block = hid_v[:, lanes_of].astype(F32) * lax.rsqrt(mean_square + EPSILON) * gain_v[:, lanes_of]
    block = jnp.where(c == 1, pltpu.roll(block, LANES // 2, 1), block)
    local[1].wait()
    query = jnp.dot(
        block[:, : LANES // 2].astype(BF16), wq_v[...], preferred_element_type=F32
    )
    own_q = qz.at[0]
    stage = qz.at[1]
    for zz in range(nz):
        stage[zz] = query[:, zz * LANES : (zz + 1) * LANES]
    own_q[z] = stage[z]
    pl.semaphore_wait(barrier, len(peers))
    base = fresh("recv", nz)
    for dz in far:
        copy_to(stage.at[zat(dz)], own_q.at[z], base + z, mp(zat(dz), x, c))
    key_base = fresh("recv", nz)
    for dz in far:
        cols = pl.ds(pl.multiple_of(zat(dz) * LANES, LANES), LANES)
        copy_to(w_key.at[:, cols], kw.at[z, c], key_base + z, mp(zat(dz), x, c))
    value_base = fresh("recv", nz)
    for dz in far:
        cols = pl.ds(pl.multiple_of(zat(dz) * LANES, LANES), LANES)
        copy_to(w_value.at[:, cols], vw.at[z, c], value_base + z, mp(zat(dz), x, c))

    local[3].wait()
    table_rows = batch
    ids = jnp.concatenate([bk_v[...], bk_v[...]], axis=1)
    row_b = lax.broadcasted_iota(jnp.int32, (batch, LANES), 0)
    lane = lax.broadcasted_iota(jnp.int32, (batch, LANES), 1)
    lens = jnp.zeros((batch, LANES), jnp.int32)
    for b in range(batch):
        lens = jnp.where(row_b == b, src_len[b], lens)
    per = LANES // 2
    position = me * per + lax.rem(lane, per)
    live = (position < lens) & (lane // per == lax.rem(row_b, 2))

    def add_bucket(k, rows):
        hit = ids == k
        return tuple(
            jnp.where(hit, table[h, k], row) for h, row in enumerate(rows)
        )

    rows = lax.fori_loop(
        0,
        table.shape[1],
        add_bucket,
        tuple(jnp.zeros((batch, LANES), F32) for _ in range(NC * nz)),
    )
    for cc in range(NC):
        for zz in range(nz):
            add_v[pl.ds((cc * nz + zz) * batch, batch), :] = rows[NC * zz + cc]

    for dz in near[::-1]:
        landed(own_q.at[zat(dz)], base + zat(dz))
    pair = functools.reduce(jnp.add, [own_q[zz] for zz in range(nz)])
    qx[x, c] = pair
    base = fresh("recv", NX * NC)
    for dx in (2, 1, 3, 0):
        for cc in range(NC):
            peer_c = lax.rem(c + cc, NC)
            if dx or cc:
                copy_to(qx.at[x, c], qx.at[x, c], base + x * NC + c, mp(z, xat(dx), peer_c))

    local[5].wait()
    for dz in far:
        landed(kw.at[zat(dz), c], key_base + zat(dz))
    sib_base = fresh("recv", 2)
    copy_to(kw.at[:, c], kw.at[:, c], sib_base, mp(z, x, other))

    for dx in range(NX):
        for cc in range(NC):
            peer_c = lax.rem(c + cc, NC)
            if dx or cc:
                landed(qx.at[xat(dx), peer_c], base + xat(dx) * NC + peer_c)
    pair = functools.reduce(
        jnp.add, [qx[xx, cc] for xx in range(NX) for cc in range(NC)]
    ).astype(BF16).astype(F32)
    pair = jnp.where(lane // per == c, pair * (float(per) ** -0.5), 0.0).astype(BF16)
    landed(kw.at[:, other], sib_base)
    mine = lax.dot_general(
        pair, kw[...].reshape(width, LANES), NT, preferred_element_type=F32
    )
    probe[x, c, z] = mine.astype(BF16)

    z_base = fresh("recv", nz)
    for dz in far:
        copy_to(probe.at[x, c, z], probe.at[x, c, z], z_base + z, mp(zat(dz), x, c))
    right_base = fresh("recv", nz)
    left_base = fresh("recv", nz)
    fwd_base = fresh("recv", nz)
    core_base = fresh("recv", NX)
    order = [0] + near

    def along_x(dz):
        zz = zat(dz)
        copy_to(probe.at[x, c, zz], probe.at[x, c, zz], right_base + zz, mp(zz * 0 + z, xat(1), c))
        copy_to(probe.at[x, c, zz], probe.at[x, c, zz], left_base + zz, mp(zz * 0 + z, xat(3), c))

    def relay(n, dz):
        zz = zat(dz)
        if n % 2 == 0:
            landed(probe.at[xat(3), c, zz], right_base + zz)
            copy_to(probe.at[xat(3), c, zz], probe.at[xat(3), c, zz], fwd_base + zz, mp(z, xat(1), c))
        else:
            landed(probe.at[xat(1), c, zz], left_base + zz)
            copy_to(probe.at[xat(1), c, zz], probe.at[xat(1), c, zz], fwd_base + zz, mp(z, xat(3), c))

    along_x(0)
    for n, dz in enumerate(order[1:]):
        landed(probe.at[x, c, zat(dz)], z_base + zat(dz))
        along_x(dz)
    copy_to(probe.at[x, c], probe.at[x, c], core_base + x, mp(z, x, other))
    for n, dz in enumerate(order):
        relay(n, dz)
    for n, dz in enumerate(order):
        zz = zat(dz)
        if n % 2 == 0:
            landed(probe.at[xat(1), c, zz], left_base + zz)
        else:
            landed(probe.at[xat(3), c, zz], right_base + zz)
    for dx in (1, 3):
        copy_to(probe.at[xat(dx), c], probe.at[xat(dx), c], core_base + xat(dx), mp(z, xat(0), other))

    def columns_in(xx):
        pltpu.make_async_copy(enc_v.at[xx], enc_v.at[xx], enc_sem.at[xx]).wait()

    for xx in range(NX):
        columns_in(xx)

    def score_part(xx):
        rows_in = jnp.concatenate(
            [probe[xx, cc, zz].astype(F32) for cc in range(NC) for zz in range(nz)], axis=0
        ).astype(BF16)
        return lax.dot_general(rows_in, enc_v[xx], NT, preferred_element_type=F32)

    landed(probe.at[x, other], core_base + x)
    scores = score_part(x)
    for n, dz in enumerate(order):
        zz = zat(dz)
        landed(probe.at[xat(2), c, zz], fwd_base + zz)
    copy_to(probe.at[xat(2), c], probe.at[xat(2), c], core_base + xat(2), mp(z, x, other))
    for dx in (1, 3, 2):
        landed(probe.at[xat(dx), other], core_base + xat(dx))
        scores = scores + score_part(xat(dx))

    heads = NC * nz
    n_rows = heads * batch
    blocks = scores.shape[1] // LANES
    row_all = lax.rem(lax.broadcasted_iota(jnp.int32, (n_rows, LANES), 0), batch)
    picked = jnp.zeros((n_rows, LANES), F32)
    for k in range(blocks):
        picked = jnp.where(row_all // 2 == k, scores[:, k * LANES : (k + 1) * LANES], picked)
    alive = jnp.concatenate([live.astype(F32)] * heads, axis=0) > 0.5
    picked = jnp.where(alive, picked + add_v[...], NEGATIVE)
    top = jnp.max(picked, axis=1, keepdims=True)
    weights = jnp.where(alive, jnp.exp(picked - top), 0.0).astype(BF16).astype(F32)
    total = jnp.sum(weights, axis=1, keepdims=True)
    spread = jnp.concatenate(
        [jnp.where(row_all // 2 == k, weights, 0.0) for k in range(blocks)], axis=1
    ).astype(BF16)
    stats = pack_stats(top, total).astype(BF16)
    per_core = nz * batch

    core_base = fresh("recv", NX)
    for dx in (2, 1, 3, 0):
        xx = xat(dx)
        mixed = jnp.dot(spread, enc_v[xx], preferred_element_type=F32).astype(BF16)
        for cc in range(NC):
            mix[cc, xx, :, pl.ds(0, width)] = mixed[cc * per_core : (cc + 1) * per_core]
            mix[cc, xx, :, pl.ds(width, LANES)] = stats[cc * per_core : (cc + 1) * per_core]
        copy_to(mix.at[other, xx], sib.at[xx], core_base + xx, mp(z, x, other))

    def both_cores(xx):
        landed(sib.at[xx], core_base + xx)
        return merged([opened(mix[c, xx], width), opened(sib[xx], width)])

    mid = per_core // 2
    half_base = fresh("recv", 2)
    hop_base = fresh("recv", 4)
    far_part = closed(both_cores(xat(2)))
    half[0, 0] = far_part[:mid]
    half[0, 1] = far_part[mid:]
    copy_to(half.at[0, 0], half.at[1, 0], half_base, mp(z, xat(1), c))
    copy_to(half.at[0, 1], half.at[1, 1], half_base + 1, mp(z, xat(3), c))

    right_part = both_cores(xat(1))
    right_low = closed(tuple(p[mid:] for p in right_part))
    hop[0, 0, 1] = right_low
    copy_to(hop.at[0, 0, 1], hop.at[1, 0, 1], hop_base + 1, mp(z, xat(1), c))
    left_part = both_cores(xat(3))
    hop[0, 1, 0] = closed(tuple(p[:mid] for p in left_part))
    copy_to(hop.at[0, 1, 0], hop.at[1, 1, 0], hop_base + 2, mp(z, xat(3), c))

    landed(half.at[1, 0], half_base)
    hop[0, 0, 0] = closed(
        merged([tuple(p[:mid] for p in right_part), opened(half[1, 0], width)])
    )
    copy_to(hop.at[0, 0, 0], hop.at[1, 0, 0], hop_base, mp(z, xat(1), c))
    landed(half.at[1, 1], half_base + 1)
    hop[0, 1, 1] = closed(
        merged([tuple(p[mid:] for p in left_part), opened(half[1, 1], width)])
    )
    copy_to(hop.at[0, 1, 1], hop.at[1, 1, 1], hop_base + 3, mp(z, xat(3), c))

    local[6].wait()
    for dz in far:
        landed(vw.at[zat(dz), c], value_base + zat(dz))
    copy_to(vw.at[:, c], vw.at[:, c], sib_base + 1, mp(z, x, other))

    own = both_cores(xat(0))
    for part, (first, second) in enumerate(((1, 2), (0, 3))):
        pass
    landed(hop.at[1, 0, 1], hop_base + 1)
    landed(hop.at[1, 1, 0], hop_base + 2)
    landed(hop.at[1, 0, 0], hop_base)
    landed(hop.at[1, 1, 1], hop_base + 3)
    for part in range(2):
        rows_of = slice(part * mid, (part + 1) * mid)
        done = merged(
            [
                tuple(p[rows_of] for p in own),
                opened(hop[1, 0, part], width),
                opened(hop[1, 1, part], width),
            ]
        )
        packed = closed(done)
        for k in range(nz // 2):
            zsend[part * (nz // 2) + k] = packed[k * batch : (k + 1) * batch]
    z_base = fresh("recv", nz)
    for dz in far:
        copy_to(zsend.at[zat(dz)], zrecv.at[z], z_base + z, mp(zat(dz), x, c))
    parts = [opened(zsend[z], width)]
    for dz in far:
        landed(zrecv.at[zat(dz)], z_base + zat(dz))
    for dz in far:
        parts.append(opened(zrecv[zat(dz)], width))
    data, _, total = merged(parts)
    mean = (data / total).astype(BF16)

    landed(vw.at[:, other], sib_base + 1)
    context = jnp.dot(mean, vw[...].reshape(width, LANES), preferred_element_type=F32)
    cx[x] = jnp.where(lane // per == c, context, 0.0)
    x_base = fresh("recv", NX)
    for dx in (2, 1, 3):
        copy_to(cx.at[x], cx.at[x], x_base + x, mp(z, xat(dx), c))
    for dx in (1, 3, 2):
        landed(cx.at[xat(dx)], x_base + xat(dx))
    cz[z, c] = functools.reduce(jnp.add, [cx[xx] for xx in range(NX)]).astype(BF16)
    base = fresh("recv", nz * NC)
    for dz in far + [0]:
        for cc in range(NC):
            peer_c = lax.rem(c + cc, NC)
            if dz or cc:
                copy_to(cz.at[z, c], cz.at[z, c], base + z * NC + c, mp(zat(dz), x, peer_c))
    for dz in [0] + near:
        for cc in range(NC):
            peer_c = lax.rem(c + cc, NC)
            if dz or cc:
                landed(cz.at[zat(dz), peer_c], base + zat(dz) * NC + peer_c)
    full = jnp.concatenate(
        [cz[zz, 0].astype(F32) + cz[zz, 1].astype(F32) for zz in range(nz)], axis=1
    ).astype(BF16)
    local[4].wait()
    yo[my_y] = lax.dot_general(full, wo_v[...], NT, preferred_element_type=F32)
    base = fresh("recv", ny)
    for dy in sorted(range(1, ny), key=lambda d: -min(d, ny - d)):
        peer = lax.rem(my_y + dy, ny)
        copy_to(yo.at[my_y], yo.at[my_y], base + my_y, {"head": peer})
    for dy in range(1, ny):
        peer = lax.rem(my_y + dy, ny)
        landed(yo.at[peer], base + peer)
    out[...] = functools.reduce(jnp.add, [yo[k] for k in range(ny)])
    for copy in sends:
        copy.wait_send()
    assert counts["send"] <= n_send and counts["recv"] <= n_recv, counts


def shards(
    nz, ny, hidden, norm_gain, w_query, enc, w_key, w_value, w_out, bias_table, buckets, src_len
):
    batch, src_local, model = enc.shape
    rows, inner = w_key.shape
    cols = w_out.shape[1]
    width = nz * LANES
    per_core = nz * batch
    n_send, n_recv = 128, 192
    me = lax.axis_index("mp")
    any_space = pl.BlockSpec(memory_space=pl.ANY)
    smem = pl.BlockSpec(memory_space=pltpu.SMEM)
    summed = pl.pallas_call(
        functools.partial(kernel, nz, ny, n_send, n_recv),
        out_shape=jax.ShapeDtypeStruct((batch, cols), F32),
        in_specs=[smem, smem] + [any_space] * 8,
        out_specs=pl.BlockSpec(memory_space=pltpu.VMEM),
        scratch_shapes=[
            pltpu.VMEM((batch, model), BF16),
            pltpu.VMEM((1, model), F32),
            pltpu.VMEM((rows, inner), BF16),
            pltpu.VMEM((cols, inner), BF16),
            pltpu.VMEM((batch, src_local), jnp.int32),
            pltpu.VMEM((NX, batch * src_local, width), BF16),
            pltpu.VMEM((nz, NC, rows, LANES), BF16),
            pltpu.VMEM((nz, NC, rows, LANES), BF16),
            pltpu.VMEM((2, nz, batch, LANES), F32),
            pltpu.VMEM((NX, NC, batch, LANES), F32),
            pltpu.VMEM((NX, NC, nz, batch, width), BF16),
            pltpu.VMEM((NC * per_core, LANES), F32),
            pltpu.VMEM((NC, NX, per_core, width + LANES), BF16),
            pltpu.VMEM((NX, per_core, width + LANES), BF16),
            pltpu.VMEM((2, 2, per_core // 2, width + LANES), BF16),
            pltpu.VMEM((2, 2, 2, per_core // 2, width + LANES), BF16),
            pltpu.VMEM((nz, batch, width + LANES), BF16),
            pltpu.VMEM((nz, batch, width + LANES), BF16),
            pltpu.VMEM((NX, batch, LANES), F32),
            pltpu.VMEM((nz, NC, batch, LANES), BF16),
            pltpu.VMEM((ny, batch, cols), F32),
            pltpu.SemaphoreType.DMA((8,)),
            pltpu.SemaphoreType.DMA((NX,)),
            pltpu.SemaphoreType.DMA((n_send,)),
            pltpu.SemaphoreType.DMA((n_recv,)),
        ],
        compiler_params=pltpu.CompilerParams(
            collective_id=0, has_side_effects=True, vmem_limit_bytes=48 * 1024 * 1024
        ),
        name="attend",
    )(
        bias_table.T,
        src_len,
        hidden,
        norm_gain.reshape(1, model),
        w_query,
        enc.reshape(batch * src_local, model),
        w_key,
        w_value,
        w_out.T,
        buckets,
    )
    residual = lax.dynamic_slice_in_dim(hidden, me * cols, cols, 1).astype(F32)
    return (summed + residual).astype(BF16)


def solution(mesh):
    ny = mesh.shape["head"]
    nz = mesh.shape["mp"] // (NX * NC)
    in_specs = (
        P(),
        P(),
        P("mp", "head"),
        P(None, "mp", None),
        P("mp", "head"),
        P("mp", "head"),
        P("head", "mp"),
        P(None, "head"),
        P(None, "mp"),
        P(),
    )
    return jax.shard_map(
        functools.partial(shards, nz, ny),
        mesh=mesh,
        in_specs=in_specs,
        out_specs=P(None, "mp"),
        check_vma=False,
    )
```

```python
import functools

import jax
import jax.numpy as jnp
from jax import lax
from jax.experimental import pallas as pl
from jax.experimental.pallas import tpu as pltpu
from jax.sharding import PartitionSpec as P

EPSILON = 1e-06
NEGATIVE = -1e30
NX = 4
NC = 2
LANES = 128
MESH = pl.DeviceIdType.MESH
F32 = jnp.float32
BF16 = jnp.bfloat16
NT = (((1,), (1,)), ((), ()))


def split3(value):
    first = value.astype(BF16).astype(F32)
    second = (value - first).astype(BF16).astype(F32)
    return first, second, value - first - second


def pack_stats(top, total):
    parts = split3(top) + split3(total)
    lane = lax.broadcasted_iota(jnp.int32, (top.shape[0], LANES), 1) // 16
    out = jnp.zeros((top.shape[0], LANES), F32)
    for k, part in enumerate(parts):
        out = jnp.where(lane == k, part, out)
    return out


def unpack_stats(stats):
    col = [stats[:, 16 * k : 16 * k + 1] for k in range(6)]
    return col[0] + col[1] + col[2], col[3] + col[4] + col[5]


def opened(block, width):
    block = block.astype(F32)
    return (block[:, :width], *unpack_stats(block[:, width:]))


def merged(parts):
    top = functools.reduce(jnp.maximum, [p[1] for p in parts])
    scales = [jnp.exp(p[1] - top) for p in parts]
    data = functools.reduce(jnp.add, [p[0] * s for p, s in zip(parts, scales)])
    total = functools.reduce(jnp.add, [p[2] * s for p, s in zip(parts, scales)])
    return data, top, total


def closed(part):
    data, top, total = part
    return jnp.concatenate([data, pack_stats(top, total)], axis=1).astype(BF16)


def kernel(
    nz,
    ny,
    n_send,
    n_recv,
    table_in,
    len_in,
    hidden,
    gain,
    w_query,
    enc,
    w_key,
    w_value,
    w_out,
    buckets,
    out,
    table,
    src_len,
    hid_v,
    gain_v,
    wq_v,
    wo_v,
    bk_v,
    enc_v,
    kw,
    vw,
    q_stage,
    qz,
    qx,
    probe,
    add_v,
    mix,
    sib,
    half,
    hop,
    zsend,
    zrecv,
    cx,
    cz,
    yo,
    local_sem,
    enc_sem,
    send_sem,
    recv_sem,
):
    batch = hid_v.shape[0]
    width = nz * LANES
    me = lax.axis_index("mp")
    my_y = lax.axis_index("head")
    z = me // (NX * NC)
    x = lax.rem(me // NC, NX)
    c = lax.rem(me, NC)
    other = 1 - c

    def mp(zz, xx, cc):
        return {"mp": (zz * NX + xx) * NC + cc}

    def zat(dz):
        return lax.rem(z + dz, nz)

    def xat(dx):
        return lax.rem(x + dx, NX)

    def piece(xx, cc, zz):
        return (xx * NC + cc) * nz + zz

    far = sorted(range(1, nz), key=lambda d: -min(d, nz - d))
    near = far[::-1]
    counts = {"send": 0, "recv": 0}
    sent = []

    def fresh(kind, number=1):
        first = counts[kind]
        counts[kind] += number
        return first

    def describe(src, dst, send, recv, device):
        return pltpu.make_async_remote_copy(
            src_ref=src,
            dst_ref=dst,
            send_sem=send_sem.at[send],
            recv_sem=recv_sem.at[recv],
            device_id=device,
            device_id_type=MESH,
        )

    def copy_to(src, dst, send, recv, device):
        describe(src, dst, send, recv, device).start()

    def landed(dst, recv):
        describe(dst, dst, 0, recv, {"mp": me}).wait_recv()

    def sending(whole):
        number = fresh("send")
        sent.append((whole, number))
        return number

    first = [(hidden, hid_v), (w_query, wq_v), (gain, gain_v)]
    cols = pl.ds(pl.multiple_of(z * LANES, LANES), LANES)
    later = [
        (w_key.at[:, cols], kw.at[z, c]),
        (w_value.at[:, cols], vw.at[z, c]),
        (buckets, bk_v),
        (table_in, table),
        (len_in, src_len),
        (w_out, wo_v),
    ]
    local = [
        pltpu.make_async_copy(src, dst, local_sem.at[k]) for k, (src, dst) in enumerate(first + later)
    ]
    for copy in local[:3]:
        copy.start()

    barrier = pltpu.get_barrier_semaphore()
    peers = [mp(zat(dz), x, cc) for dz in far for cc in (0, 1)]
    peers += [mp(z, xat(dx), cc) for dx in range(1, NX) for cc in (0, 1)]
    peers += [mp(z, x, other)]
    peers += [{"head": lax.rem(my_y + dy, ny)} for dy in range(1, ny)]
    for peer in peers:
        pl.semaphore_signal(barrier, inc=1, device_id=peer, device_id_type=MESH)

    local[0].wait()
    wide = hid_v[...].astype(F32)
    mean_square = jnp.mean(wide * wide, axis=-1, keepdims=True)
    local[2].wait()
    lanes_of = pl.ds(pl.multiple_of((z * NX + x) * LANES, LANES), LANES)
    block = hid_v[:, lanes_of].astype(F32) * lax.rsqrt(mean_square + EPSILON) * gain_v[:, lanes_of]
    block = jnp.where(c == 1, pltpu.roll(block, LANES // 2, 1), block)
    local[1].wait()
    query = jnp.dot(block[:, : LANES // 2].astype(BF16), wq_v[...], preferred_element_type=F32)
    for zz in range(nz):
        q_stage[zz] = query[:, zz * LANES : (zz + 1) * LANES]
    qz[z] = q_stage[z]
    pl.semaphore_wait(barrier, len(peers))
    send, qz_recv = sending(q_stage.at[pl.ds(0, nz - 1)]), fresh("recv")
    for dz in far:
        copy_to(q_stage.at[zat(dz)], qz.at[z], send, qz_recv, mp(zat(dz), x, c))
    blocks_recv = []
    for source, target in ((w_key, kw), (w_value, vw)):
        send, recv = sending(target.at[pl.ds(0, nz - 1), 0]), fresh("recv")
        blocks_recv.append(recv)
        for dz in far:
            cols = pl.ds(pl.multiple_of(zat(dz) * LANES, LANES), LANES)
            copy_to(source.at[:, cols], target.at[z, c], send, recv, mp(zat(dz), x, c))
    for copy in local[3:]:
        copy.start()
    for xx in range(NX):
        for zz in range(nz):
            pltpu.make_async_copy(
                enc.at[:, pl.ds((zz * NX + xx) * LANES, LANES)],
                enc_v.at[xx, :, pl.ds(zz * LANES, LANES)],
                enc_sem.at[xx],
            ).start()

    for copy in local[5:8]:
        copy.wait()
    ids = jnp.concatenate([bk_v[...], bk_v[...]], axis=1)
    row_b = lax.broadcasted_iota(jnp.int32, (batch, LANES), 0)
    lane = lax.broadcasted_iota(jnp.int32, (batch, LANES), 1)
    lens = jnp.zeros((batch, LANES), jnp.int32)
    for b in range(batch):
        lens = jnp.where(row_b == b, src_len[b], lens)
    per = LANES // 2
    position = me * per + lax.rem(lane, per)
    live = (position < lens) & (lane // per == lax.rem(row_b, 2))

    def add_bucket(k, rows):
        hit = ids == k
        return tuple(jnp.where(hit, table[h, k], row) for h, row in enumerate(rows))

    rows = lax.fori_loop(
        0,
        table.shape[1],
        add_bucket,
        tuple(jnp.zeros((batch, LANES), F32) for _ in range(NC * nz)),
    )
    for cc in range(NC):
        for zz in range(nz):
            add_v[pl.ds((cc * nz + zz) * batch, batch), :] = rows[NC * zz + cc]

    landed(qz.at[pl.ds(0, nz - 1)], qz_recv)
    qx[x * NC + c] = functools.reduce(jnp.add, [qz[zz] for zz in range(nz)])
    n_plane = NX * NC
    send, recv = sending(qx.at[pl.ds(0, n_plane - 1)]), fresh("recv")
    for dx in (2, 1, 3, 0):
        for dc in range(NC):
            if dx or dc:
                copy_to(
                    qx.at[x * NC + c],
                    qx.at[x * NC + c],
                    send,
                    recv,
                    mp(z, xat(dx), lax.rem(c + dc, NC)),
                )
    local[3].wait()
    landed(kw.at[pl.ds(0, nz - 1), c], blocks_recv[0])
    key_sib = fresh("recv")
    copy_to(kw.at[:, c], kw.at[:, c], sending(kw.at[:, c]), key_sib, mp(z, x, other))
    landed(qx.at[pl.ds(0, n_plane - 1)], recv)
    pair = functools.reduce(jnp.add, [qx[k] for k in range(n_plane)]).astype(BF16).astype(F32)
    pair = jnp.where(lane // per == c, pair * (float(per) ** -0.5), 0.0).astype(BF16)
    landed(kw.at[:, other], key_sib)
    mine = lax.dot_general(pair, kw[...].reshape(width, LANES), NT, preferred_element_type=F32)
    probe[piece(x, c, z)] = mine.astype(BF16)

    total_pieces = (nz - 1) + 2 * nz + nz + NX * nz
    send = sending(probe.at[pl.ds(0, total_pieces)])
    z_recv, right_recv, left_recv = fresh("recv", nz), fresh("recv", nz), fresh("recv", nz)
    relay_recv, core_recv = fresh("recv", nz), fresh("recv", NX)
    order = [0] + near

    def pass_on(xx, zz, recv, device):
        spot = probe.at[piece(xx, c, zz)]
        copy_to(spot, spot, send, recv, device)

    def on_z(n, dz):
        zz = zat(dz)
        if dz:
            landed(probe.at[piece(x, c, zz)], z_recv + zz)
        pass_on(x, zz, right_recv + zz, mp(z, xat(1), c))
        pass_on(x, zz, left_recv + zz, mp(z, xat(3), c))
        pass_on(x, zz, core_recv + x, mp(z, x, other))

    def on_x(n, dz):
        zz = zat(dz)
        for dx, recv, back, here in ((3, right_recv, 1, n % 2 == 0), (1, left_recv, 3, n % 2 == 1)):
            landed(probe.at[piece(xat(dx), c, zz)], recv + zz)
            if here:
                pass_on(xat(dx), zz, relay_recv + zz, mp(z, xat(back), c))
            pass_on(xat(dx), zz, core_recv + xat(dx), mp(z, x, other))

    def on_relay(n, dz):
        zz = zat(dz)
        landed(probe.at[piece(xat(2), c, zz)], relay_recv + zz)
        pass_on(xat(2), zz, core_recv + xat(2), mp(z, x, other))

    def score_part(xx):
        landed(probe.at[pl.ds(piece(xx, other, 0), nz)], core_recv + xx)
        rows_in = jnp.concatenate(
            [probe[piece(xx, cc, zz)].astype(F32) for cc in range(NC) for zz in range(nz)], axis=0
        ).astype(BF16)
        return lax.dot_general(rows_in, enc_v[xx], NT, preferred_element_type=F32)

    for dz in near:
        pass_on(x, z, z_recv + z, mp(zat(dz), x, c))
    lag = 5
    for n in range(nz + lag):
        if n < nz:
            on_z(n, order[n])
        if n >= lag:
            on_x(n - lag, order[n - lag])
    for xx in range(NX):
        pltpu.make_async_copy(enc_v.at[xx], enc_v.at[xx], enc_sem.at[xx]).wait()
    scores = score_part(x)
    for n, dz in enumerate(order[:-2]):
        on_relay(n, dz)
    for dx in (1, 3):
        scores = scores + score_part(xat(dx))
    for n, dz in list(enumerate(order))[-2:]:
        on_relay(n, dz)
    scores = scores + score_part(xat(2))

    heads = NC * nz
    n_rows = heads * batch
    blocks = scores.shape[1] // LANES
    row_all = lax.rem(lax.broadcasted_iota(jnp.int32, (n_rows, LANES), 0), batch)
    picked = jnp.zeros((n_rows, LANES), F32)
    for k in range(blocks):
        picked = jnp.where(row_all // 2 == k, scores[:, k * LANES : (k + 1) * LANES], picked)
    alive = jnp.concatenate([live.astype(F32)] * heads, axis=0) > 0.5
    picked = jnp.where(alive, picked + add_v[...], NEGATIVE)
    top = jnp.max(picked, axis=1, keepdims=True)
    weights = jnp.where(alive, jnp.exp(picked - top), 0.0).astype(BF16).astype(F32)
    total = jnp.sum(weights, axis=1, keepdims=True)
    spread = jnp.concatenate(
        [jnp.where(row_all // 2 == k, weights, 0.0) for k in range(blocks)], axis=1
    ).astype(BF16)
    stats = pack_stats(top, total).astype(BF16)
    per_core = nz * batch

    core_recv = fresh("recv", NX)
    mix_send = sending(sib)

    def mix_part(dx):
        xx = xat(dx)
        mixed = jnp.dot(spread, enc_v[xx], preferred_element_type=F32).astype(BF16)
        for cc in range(NC):
            mix[cc, xx, :, pl.ds(0, width)] = mixed[cc * per_core : (cc + 1) * per_core]
            mix[cc, xx, :, pl.ds(width, LANES)] = stats[cc * per_core : (cc + 1) * per_core]
        copy_to(mix.at[other, xx], sib.at[xx], mix_send, core_recv + xx, mp(z, x, other))

    def both_cores(xx):
        landed(sib.at[xx], core_recv + xx)
        return merged([opened(mix[c, xx], width), opened(sib[xx], width)])

    n_group = min(4, nz)
    size = per_core // n_group
    ways = (1, 3)
    split = [range(n_group // 2), range(n_group // 2, n_group)]
    half_send, half_recv = sending(half.at[0]), fresh("recv", n_group)
    hop_send, hop_recv = sending(hop.at[0]), fresh("recv", 2 * n_group)

    def rows_of(part, group):
        return tuple(p[group * size : (group + 1) * size] for p in part)

    def hop_on(way, group, part):
        hop[0, way, group] = closed(part)
        copy_to(
            hop.at[0, way, group],
            hop.at[1, way, group],
            hop_send,
            hop_recv + way * n_group + group,
            mp(z, xat(ways[way]), c),
        )

    def hop_landed(way, group):
        landed(hop.at[1, way, group], hop_recv + way * n_group + group)
        return opened(hop[1, way, group], width)

    mix_part(2)
    mix_part(1)
    mix_part(3)
    landed(sib.at[xat(2)], core_recv + xat(2))
    for way, group in [(w, g) for k in range(n_group // 2) for w, g in ((0, split[0][k]), (1, split[1][k]))]:
        span = pl.ds(group * size, size)
        half[0, group] = closed(
            merged([opened(mix[c, xat(2), span], width), opened(sib[xat(2), span], width)])
        )
        copy_to(
            half.at[0, group],
            half.at[1, group],
            half_send,
            half_recv + group,
            mp(z, xat(ways[way]), c),
        )

    near_parts = []
    for way in range(2):
        near_parts.append(both_cores(xat(ways[way])))
        for group in split[1 - way]:
            hop_on(way, group, rows_of(near_parts[way], group))
    mix_part(0)
    for k in range(n_group // 2):
        for way in range(2):
            group = split[way][k]
            landed(half.at[1, group], half_recv + group)
            hop_on(
                way,
                group,
                merged([rows_of(near_parts[way], group), opened(half[1, group], width)]),
            )
    local[4].wait()
    landed(vw.at[pl.ds(0, nz - 1), c], blocks_recv[1])
    value_sib = fresh("recv")
    copy_to(vw.at[:, c], vw.at[:, c], sending(vw.at[:, c]), value_sib, mp(z, x, other))
    own = both_cores(xat(0))
    z_send, z_recv = sending(zsend.at[pl.ds(0, nz - 1)]), fresh("recv")
    sums = {}
    for way in range(2):
        for group in split[1 - way]:
            sums[group] = merged([rows_of(own, group), hop_landed(way, group)])
    per_group = nz // n_group
    for k in range(n_group // 2):
        for way in range(2):
            group = split[way][k]
            packed = closed(merged([sums[group], hop_landed(way, group)]))
            for m in range(per_group):
                zsend[group * per_group + m] = packed[m * batch : (m + 1) * batch]
    for dz in far:
        copy_to(zsend.at[zat(dz)], zrecv.at[z], z_send, z_recv, mp(zat(dz), x, c))
    parts = [opened(zsend[z], width)]
    landed(zrecv.at[pl.ds(0, nz - 1)], z_recv)
    for dz in far:
        parts.append(opened(zrecv[zat(dz)], width))
    data, _, total = merged(parts)
    mean = (data / total).astype(BF16)

    landed(vw.at[:, other], value_sib)
    context = jnp.dot(mean, vw[...].reshape(width, LANES), preferred_element_type=F32)
    cx[x * NC + c] = jnp.where(lane // per == c, context, 0.0)
    send, recv = sending(cx.at[pl.ds(0, n_plane - 1)]), fresh("recv")
    for dx in (2, 1, 3, 0):
        for dc in range(NC):
            if dx or dc:
                copy_to(
                    cx.at[x * NC + c],
                    cx.at[x * NC + c],
                    send,
                    recv,
                    mp(z, xat(dx), lax.rem(c + dc, NC)),
                )
    landed(cx.at[pl.ds(0, n_plane - 1)], recv)
    cz[z] = functools.reduce(jnp.add, [cx[k] for k in range(n_plane)]).astype(BF16)
    send, recv = sending(cz.at[pl.ds(0, nz - 1)]), fresh("recv")
    for dz in far:
        copy_to(cz.at[z], cz.at[z], send, recv, mp(zat(dz), x, c))
    local[8].wait()
    landed(cz.at[pl.ds(0, nz - 1)], recv)
    full = jnp.concatenate([cz[zz] for zz in range(nz)], axis=1)
    yo[my_y] = lax.dot_general(full, wo_v[...], NT, preferred_element_type=F32)
    if ny > 1:
        send, recv = sending(yo.at[pl.ds(0, ny - 1)]), fresh("recv")
        for dy in sorted(range(1, ny), key=lambda d: -min(d, ny - d)):
            copy_to(yo.at[my_y], yo.at[my_y], send, recv, {"head": lax.rem(my_y + dy, ny)})
        landed(yo.at[pl.ds(0, ny - 1)], recv)
    out[...] = functools.reduce(jnp.add, [yo[k] for k in range(ny)])
    for whole, number in sent:
        describe(whole, whole, number, 0, {"mp": me}).wait_send()
    assert counts["send"] <= n_send and counts["recv"] <= n_recv, counts


def shards(
    nz, ny, hidden, norm_gain, w_query, enc, w_key, w_value, w_out, bias_table, buckets, src_len
):
    batch, src_local, model = enc.shape
    rows, inner = w_key.shape
    cols = w_out.shape[1]
    width = nz * LANES
    per_core = nz * batch
    n_group = min(4, nz)
    n_send, n_recv = 14, 10 + 4 * nz + 2 * NX + 3 * n_group
    me = lax.axis_index("mp")
    any_space = pl.BlockSpec(memory_space=pltpu.HBM)
    summed = pl.pallas_call(
        functools.partial(kernel, nz, ny, n_send, n_recv),
        out_shape=jax.ShapeDtypeStruct((batch, cols), F32),
        in_specs=[any_space] * 10,
        out_specs=pl.BlockSpec(memory_space=pltpu.VMEM),
        scratch_shapes=[
            pltpu.SMEM(bias_table.shape[::-1], F32),
            pltpu.SMEM(src_len.shape, jnp.int32),
            pltpu.VMEM((batch, model), BF16),
            pltpu.VMEM((1, model), F32),
            pltpu.VMEM((rows, inner), BF16),
            pltpu.VMEM((cols, inner), BF16),
            pltpu.VMEM((batch, src_local), jnp.int32),
            pltpu.VMEM((NX, batch * src_local, width), BF16),
            pltpu.VMEM((nz, NC, rows, LANES), BF16),
            pltpu.VMEM((nz, NC, rows, LANES), BF16),
            pltpu.VMEM((nz, batch, LANES), F32),
            pltpu.VMEM((nz, batch, LANES), F32),
            pltpu.VMEM((NX * NC, batch, LANES), F32),
            pltpu.VMEM((NX * NC * nz, batch, width), BF16),
            pltpu.VMEM((NC * per_core, LANES), F32),
            pltpu.VMEM((NC, NX, per_core, width + LANES), BF16),
            pltpu.VMEM((NX, per_core, width + LANES), BF16),
            pltpu.VMEM((2, n_group, per_core // n_group, width + LANES), BF16),
            pltpu.VMEM((2, 2, n_group, per_core // n_group, width + LANES), BF16),
            pltpu.VMEM((nz, batch, width + LANES), BF16),
            pltpu.VMEM((nz, batch, width + LANES), BF16),
            pltpu.VMEM((NX * NC, batch, LANES), F32),
            pltpu.VMEM((nz, batch, LANES), BF16),
            pltpu.VMEM((ny, batch, cols), F32),
            pltpu.SemaphoreType.DMA((9,)),
            pltpu.SemaphoreType.DMA((NX,)),
            pltpu.SemaphoreType.DMA((n_send,)),
            pltpu.SemaphoreType.DMA((n_recv,)),
        ],
        compiler_params=pltpu.CompilerParams(
            collective_id=0, has_side_effects=True, vmem_limit_bytes=67043328
        ),
        name="attend",
    )(
        bias_table.T,
        src_len,
        hidden,
        norm_gain.reshape(1, model),
        w_query,
        enc.reshape(batch * src_local, model),
        w_key,
        w_value,
        w_out.T,
        buckets,
    )
    residual = lax.dynamic_slice_in_dim(hidden, me * cols, cols, 1).astype(F32)
    return (summed + residual).astype(BF16)


def solution(mesh):
    ny = mesh.shape["head"]
    nz = mesh.shape["mp"] // (NX * NC)
    in_specs = (
        P(),
        P(),
        P("mp", "head"),
        P(None, "mp", None),
        P("mp", "head"),
        P("mp", "head"),
        P("head", "mp"),
        P(None, "head"),
        P(None, "mp"),
        P(),
    )
    return jax.shard_map(
        functools.partial(shards, nz, ny),
        mesh=mesh,
        in_specs=in_specs,
        out_specs=P(None, "mp"),
        check_vma=False,
    )
```
